32 devices in a mesh: dp: 4 (over y, z), tp: 8 (over x, core).
Axes of the slice: x: 4, y: 2, z: 2, core: 2. Of those that a mesh axis runs over, the one named last changes fastest.
The devices are a block of a 4x4x8 slice.
Arguments:
- x_in: bfloat16 [4, 3072, 3840], P('dp', 'tp'), parts along dimension 0
- positions: int32 [4, 3072], P('dp', 'tp'), parts along dimension 0
- grad_out: bfloat16 [4, 3072, 3840], P('dp', 'tp'), parts along dimension 0
- w_query: bfloat16 [3840, 16, 256], P(None, 'tp')
- w_key: bfloat16 [3840, 8, 256], P(None, 'tp')
- w_value: bfloat16 [3840, 8, 256], P(None, 'tp')
- w_out: bfloat16 [16, 256, 3840], P('tp')
- gain_pre: float32 [3840], replicated
- gain_post: float32 [3840], replicated
Outputs:
- output 1: bfloat16 [4, 3072, 3840], P('dp', 'tp'), parts along dimension 0
- output 2: bfloat16 [4, 3072, 3840], P('dp', 'tp'), parts along dimension 0
- output 3: float32 [15360, 16, 256], P('dp', 'tp'), parts along dimension 0
- output 4: float32 [15360, 8, 256], P('dp', 'tp'), parts along dimension 0
- output 5: float32 [15360, 8, 256], P('dp', 'tp'), parts along dimension 0
- output 6: float32 [64, 256, 3840], P(('dp', 'tp')), parts along dimension 0
- output 7: float32 [15360], P('dp'), parts along dimension 0
- output 8: float32 [15360], P('dp'), parts along dimension 0
There are 4 independent parts. The reference program is written for one: setup_inputs(seed, part) draws one part's arguments, and reference() takes and returns one part's arrays. A program takes and returns all parts, laid end to end along the dimension named above; an argument that names none is the same for every part.
All inputs are finite; a program needn't handle non-finite values.
Results may differ from the reference program's by a relative error of at most 0.0190443.
Values are sent between devices in bfloat16 or wider.
A program may use at most 768 MiB of HBM per device.

```python
import functools
import jax
import jax.numpy as jnp
from jax import lax

BATCH_ROWS = 1
SEQ_LEN = 3072
MODEL_DIM = 3840
NUM_HEADS = 16
KV_HEADS = 8
HEAD_DIM = 256
WINDOW = 4096
QUERY_BLOCK = 128
SOFT_CAP = 50.0
NORM_EPS = 1e-6
ROPE_THETA = 10000.0


def draw_positions(pos_key, n_rows, seq_len):
    key_off, key_hit, key_jump = jax.random.split(pos_key, 3)
    offset = jax.random.randint(key_off, (n_rows, 1), 0, WINDOW)
    hit_draw = jax.random.randint(key_hit, (n_rows, seq_len), 0, max(seq_len // 8, 1))
    jump_size = jax.random.randint(key_jump, (n_rows, seq_len), 1, 2 * WINDOW)
    pos_steps = 1 + jnp.where(hit_draw == 0, jump_size, 0)
    return (offset + jnp.cumsum(pos_steps, axis=1) - pos_steps[:, :1]).astype(jnp.int32)


def setup_inputs(seed: int = 0, part: int = 0) -> dict:
    base_key = jax.random.key(seed)
    part_key = jax.random.fold_in(base_key, part)
    key_x, key_pos, key_dy = jax.random.split(part_key, 3)
    key_q, key_k, key_v, key_o, key_gp, key_gq = jax.random.split(base_key, 6)
    act_shape = (BATCH_ROWS, SEQ_LEN, MODEL_DIM)
    in_scale = MODEL_DIM ** -0.5
    out_scale = (NUM_HEADS * HEAD_DIM) ** -0.5
    x_in = jax.random.normal(key_x, act_shape, jnp.float32).astype(jnp.bfloat16)
    positions = draw_positions(key_pos, BATCH_ROWS, SEQ_LEN)
    grad_out = jax.random.normal(key_dy, act_shape, jnp.float32).astype(jnp.bfloat16)
    w_query = (jax.random.normal(key_q, (MODEL_DIM, NUM_HEADS, HEAD_DIM), jnp.float32) * in_scale).astype(jnp.bfloat16)
    w_key = (jax.random.normal(key_k, (MODEL_DIM, KV_HEADS, HEAD_DIM), jnp.float32) * in_scale).astype(jnp.bfloat16)
    w_value = (jax.random.normal(key_v, (MODEL_DIM, KV_HEADS, HEAD_DIM), jnp.float32) * in_scale).astype(jnp.bfloat16)
    w_out = (jax.random.normal(key_o, (NUM_HEADS, HEAD_DIM, MODEL_DIM), jnp.float32) * out_scale).astype(jnp.bfloat16)
    gain_pre = 0.5 * jax.random.normal(key_gp, (MODEL_DIM,), jnp.float32)
    gain_post = 0.5 * jax.random.normal(key_gq, (MODEL_DIM,), jnp.float32)
    return {'x_in': x_in, 'positions': positions, 'grad_out': grad_out, 'w_query': w_query, 'w_key': w_key, 'w_value': w_value, 'w_out': w_out, 'gain_pre': gain_pre, 'gain_post': gain_post}


def rms_norm(hidden, scale_w):
    values = hidden.astype(jnp.float32)
    inv_rms = lax.rsqrt(jnp.mean(values * values, axis=-1, keepdims=True) + NORM_EPS)
    return (values * inv_rms * (1.0 + scale_w)).astype(jnp.bfloat16)


def rope_tables(positions, head_dim):
    half_dim = head_dim // 2
    inv_freq = ROPE_THETA ** (-2.0 * jnp.arange(half_dim, dtype=jnp.float32) / head_dim)
    angles = positions.astype(jnp.float32)[:, :, None] * inv_freq
    return jnp.cos(angles)[:, :, None, :], jnp.sin(angles)[:, :, None, :]


def apply_rope(values, cos_t, sin_t):
    half_dim = values.shape[-1] // 2
    lo_half = values[..., :half_dim]
    hi_half = values[..., half_dim:]
    return jnp.concatenate([lo_half * cos_t - hi_half * sin_t, hi_half * cos_t + lo_half * sin_t], axis=-1)


def block_probs(q_blk, k_blk, pos_q, pos_k):
    scores = jnp.einsum('bqkgd,bskd->bkgqs', q_blk.astype(jnp.float32), k_blk.astype(jnp.float32))
    capped = SOFT_CAP * jnp.tanh(scores / SOFT_CAP)
    pos_gap = pos_q[:, :, None] - pos_k[:, None, :]
    in_window = ((pos_gap >= 0) & (pos_gap < WINDOW))[:, None, None, :, :]
    return jax.nn.softmax(jnp.where(in_window, capped, -1e30), axis=-1)


def attention(q_all, k_all, v_all, positions):
    seq_len = positions.shape[1]
    q_block = min(QUERY_BLOCK, seq_len)
    slab_len = min(WINDOW + q_block, seq_len)

    def one_block(blk_idx):
        q_start = blk_idx * q_block
        k_start = jnp.maximum(q_start + q_block - slab_len, 0)
        q_blk = lax.dynamic_slice_in_dim(q_all, q_start, q_block, axis=1)
        k_blk = lax.dynamic_slice_in_dim(k_all, k_start, slab_len, axis=1)
        v_blk = lax.dynamic_slice_in_dim(v_all, k_start, slab_len, axis=1)
        pos_q = lax.dynamic_slice_in_dim(positions, q_start, q_block, axis=1)
        pos_k = lax.dynamic_slice_in_dim(positions, k_start, slab_len, axis=1)
        prob_blk = block_probs(q_blk, k_blk, pos_q, pos_k)
        out_blk = jnp.einsum('bkgqs,bskd->bqkgd', prob_blk.astype(jnp.bfloat16).astype(jnp.float32), v_blk.astype(jnp.float32))
        return out_blk.astype(jnp.bfloat16)

    blocks = lax.map(jax.checkpoint(one_block), jnp.arange(seq_len // q_block))
    return jnp.moveaxis(blocks, 0, 1).reshape(q_all.shape)


def forward(positions, x_in, w_query, w_key, w_value, w_out, gain_pre, gain_post):
    n_rows, seq_len = positions.shape
    num_heads, head_dim = w_query.shape[1], w_query.shape[2]
    kv_heads = w_key.shape[1]
    normed = rms_norm(x_in, gain_pre).astype(jnp.float32)
    cos_t, sin_t = rope_tables(positions, head_dim)
    q_lin = jnp.einsum('bsd,dhe->bshe', normed, w_query.astype(jnp.float32))
    k_lin = jnp.einsum('bsd,dhe->bshe', normed, w_key.astype(jnp.float32))
    v_lin = jnp.einsum('bsd,dhe->bshe', normed, w_value.astype(jnp.float32))
    q_all = (apply_rope(q_lin, cos_t, sin_t) * head_dim ** -0.5).astype(jnp.bfloat16)
    q_all = q_all.reshape(n_rows, seq_len, kv_heads, num_heads // kv_heads, head_dim)
    k_all = apply_rope(k_lin, cos_t, sin_t).astype(jnp.bfloat16)
    v_all = v_lin.astype(jnp.bfloat16)
    attn_out = attention(q_all, k_all, v_all, positions).reshape(n_rows, seq_len, num_heads, head_dim)
    proj_out = jnp.einsum('bshe,hed->bsd', attn_out.astype(jnp.float32), w_out.astype(jnp.float32)).astype(jnp.bfloat16)
    post_norm = rms_norm(proj_out, gain_post)
    return (x_in.astype(jnp.float32) + post_norm.astype(jnp.float32)).astype(jnp.bfloat16)


def reference(x_in, positions, grad_out, w_query, w_key, w_value, w_out, gain_pre, gain_post):
    y_out, pullback = jax.vjp(functools.partial(forward, positions), x_in, w_query, w_key, w_value, w_out, gain_pre, gain_post)
    grad_x, grad_wq, grad_wk, grad_wv, grad_wo, grad_pre, grad_post = pullback(grad_out)
    return (y_out, grad_x, grad_wq.astype(jnp.float32), grad_wk.astype(jnp.float32), grad_wv.astype(jnp.float32), grad_wo.astype(jnp.float32), grad_pre.astype(jnp.float32), grad_post.astype(jnp.float32))
```

```python
import functools

import jax
import jax.numpy as jnp
from jax import lax
from jax.experimental import pallas as pl
from jax.experimental.pallas import tpu as pltpu
from jax.sharding import PartitionSpec as P

WINDOW = 4096
SOFT_CAP = 50.0
NORM_EPS = 1e-6
ROPE_THETA = 10000.0
ROWS = 128
LOG2E = 1.4426950408889634
VMEM_LIMIT = 60 * 1024 * 1024


def rms_norm(hidden, scale_w):
    values = hidden.astype(jnp.float32)
    inv_rms = lax.rsqrt(jnp.mean(values * values, axis=-1, keepdims=True) + NORM_EPS)
    return (values * inv_rms * (1.0 + scale_w)).astype(jnp.bfloat16)


def params(n=1):
    return pltpu.CompilerParams(dimension_semantics=("arbitrary",) * n, vmem_limit_bytes=VMEM_LIMIT)


def qkv_kernel(n_heads, scale, a_ref, w_ref, cos_ref, sin_ref, q_ref, k_ref, kt_ref, v_ref, vt_ref):
    owners, n_chunks, _, d_model = a_ref.shape
    rows2 = owners * n_chunks * ROWS
    rows = n_chunks * ROWS
    lin = jnp.dot(a_ref[...].reshape(rows2, d_model), w_ref[...], preferred_element_type=jnp.float32)
    half = cos_ref.shape[-1]
    hd = 2 * half
    cos = cos_ref[...].reshape(rows2, half)
    sin = sin_ref[...].reshape(rows2, half)

    def rope(col):
        lo = lin[:, col:col + half]
        hi = lin[:, col + half:col + hd]
        return lo * cos - hi * sin, hi * cos + lo * sin

    for h in range(n_heads):
        lo, hi = rope(h * hd)
        q_ref[..., h * hd:h * hd + half] = (lo * scale).astype(jnp.bfloat16).reshape(owners, n_chunks, ROWS, half)
        q_ref[..., h * hd + half:(h + 1) * hd] = (hi * scale).astype(jnp.bfloat16).reshape(owners, n_chunks, ROWS, half)
    lo, hi = rope(n_heads * hd)
    k = jnp.concatenate([lo.astype(jnp.bfloat16), hi.astype(jnp.bfloat16)], axis=1)
    v = lin[:, (n_heads + 1) * hd:].astype(jnp.bfloat16)
    for i in range(owners):
        for c in range(n_chunks):
            at = i * rows + c * ROWS
            k_i = k[at:at + ROWS]
            v_i = v[at:at + ROWS]
            k_ref[i, c] = k_i
            kt_ref[i, c] = k_i.T
            v_ref[i, c] = v_i
            vt_ref[i, c] = v_i.T


def qkv(n_heads, scale, a, w, cos_t, sin_t):
    n_own, n_chunks, rows, d_model = a.shape
    hd = 2 * cos_t.shape[-1]
    bf = lambda s: jax.ShapeDtypeStruct((n_own, n_chunks) + s, jnp.bfloat16)
    blk = lambda s: pl.BlockSpec((1, n_chunks) + s, lambda i: (i, 0, 0, 0))
    outs = [(rows, n_heads * hd), (rows, hd), (hd, rows), (rows, hd), (hd, rows)]
    return pl.pallas_call(
        functools.partial(qkv_kernel, n_heads, scale),
        grid=(n_own,),
        in_specs=[blk((rows, d_model)), pl.BlockSpec(w.shape, lambda i: (0, 0)), blk((rows, hd // 2)), blk((rows, hd // 2))],
        out_specs=[blk(o) for o in outs],
        out_shape=[bf(o) for o in outs],
        compiler_params=params(),
        cost_estimate=pl.CostEstimate(flops=2 * a.size * w.shape[1], transcendentals=0, bytes_accessed=2 * (a.size + w.size)),
        name="qkv_rope",
    )(a, w, cos_t, sin_t)


def key_mask(posq_ref, posk_ref, blk):
    gap = posq_ref[0] - posk_ref[blk]
    return (gap >= 0) & (gap < WINDOW)


def masked_exp(t, mask, n_heads):
    e = jnp.exp2(t * (SOFT_CAP * LOG2E))
    return jnp.concatenate([jnp.where(mask, e[:, h * ROWS:(h + 1) * ROWS], 0.0) for h in range(n_heads)], axis=1)


def fwd_kernel(n_heads, lo_ref, q_ref, k_ref, vt_ref, posq_ref, posk_ref, o_ref, ot_ref, qt_ref, li_ref, acc_ref):
    own = pl.program_id(0)
    n_chunks, hd = k_ref.shape[1], k_ref.shape[3]
    q = q_ref[0, 0]
    qt = jnp.concatenate([q[:, h * hd:(h + 1) * hd].T for h in range(n_heads)], axis=1)
    qt_ref[0] = qt
    acc_ref[...] = jnp.zeros_like(acc_ref)

    def body(blk, l_sum):
        k_b = k_ref[blk].reshape(n_chunks * ROWS, hd)
        s = jnp.dot(k_b, qt_ref[0], preferred_element_type=jnp.float32)
        t = jnp.tanh(s * (1.0 / SOFT_CAP))
        e = masked_exp(t, key_mask(posq_ref, posk_ref, blk), n_heads)
        vt = jnp.concatenate([vt_ref[blk, c] for c in range(n_chunks)], axis=1)
        acc_ref[...] += jnp.dot(vt, e.astype(jnp.bfloat16), preferred_element_type=jnp.float32)
        return l_sum + jnp.sum(e, axis=0, keepdims=True)

    l_sum = lax.fori_loop(lo_ref[own], own + 1, body, jnp.zeros((1, n_heads * ROWS), jnp.float32))
    inv = 1.0 / l_sum
    li_ref[0] = inv
    ot = (acc_ref[...] * inv).astype(jnp.bfloat16)
    ot_ref[0] = ot
    for h in range(n_heads):
        o_ref[0, :, h * hd:(h + 1) * hd] = ot[:, h * ROWS:(h + 1) * ROWS].T


def attn_fwd(n_heads, chunk, lo, q, k, vt, posq, posk):
    n_own, n_chunks, rows, hd = k.shape
    lanes = n_heads * rows
    full = lambda x: pl.BlockSpec(x.shape, lambda i, lo: (0,) * x.ndim)
    per = lambda s: pl.BlockSpec((1,) + s, lambda i, lo: (i, 0, 0))
    return pl.pallas_call(
        functools.partial(fwd_kernel, n_heads),
        grid_spec=pltpu.PrefetchScalarGridSpec(
            num_scalar_prefetch=1, grid=(n_own,),
            in_specs=[pl.BlockSpec((1, 1, rows, n_heads * hd), lambda i, lo: (i, chunk, 0, 0)), full(k), full(vt), per((1, rows)), full(posk)],
            out_specs=[per((rows, n_heads * hd)), per((hd, lanes)), per((hd, lanes)), per((1, lanes))],
            scratch_shapes=[pltpu.VMEM((hd, lanes), jnp.float32)]),
        out_shape=[jax.ShapeDtypeStruct((n_own, rows, n_heads * hd), jnp.bfloat16),
                   jax.ShapeDtypeStruct((n_own, hd, lanes), jnp.bfloat16),
                   jax.ShapeDtypeStruct((n_own, hd, lanes), jnp.bfloat16),
                   jax.ShapeDtypeStruct((n_own, 1, lanes), jnp.float32)],
        compiler_params=params(),
        cost_estimate=pl.CostEstimate(flops=4 * n_own * lanes * (n_own * n_chunks * rows // 2) * hd,
                                      transcendentals=0, bytes_accessed=12 * k.size),
        name="attn_fwd",
    )(lo, q, k, vt, posq, posk)


def bwd_kernel(n_heads, scale, chunk, first, last, *refs):
    lo_ref, q_ref, qt_ref, ot_ref, li_ref, do_ref, k_ref, kt_ref, v_ref, posq_ref, posk_ref, cos_ref, sin_ref = refs[:13]
    rest = refs[13:]
    if not first:
        dki_ref, dvi_ref = rest[:2]
        rest = rest[2:]
    dq_ref, dk_out, dv_out = rest[:3]
    if last:
        dk_ref, dv_ref = rest[3:5]
        rest = rest[5:]
    else:
        dk_ref, dv_ref = dk_out, dv_out
        rest = rest[3:]
    dqt_ref, dot_ref, dos_ref, qs_ref = rest
    own = pl.program_id(0)
    n_own, n_chunks, _, hd = k_ref.shape
    half = hd // 2

    @pl.when(own == 0)
    def _():
        if first:
            dk_ref[...] = jnp.zeros_like(dk_ref)
            dv_ref[...] = jnp.zeros_like(dv_ref)
        else:
            dk_ref[...] = dki_ref[...]
            dv_ref[...] = dvi_ref[...]

    do = do_ref[0]
    q = q_ref[0, 0]
    for h in range(n_heads):
        dos_ref[h * ROWS:(h + 1) * ROWS] = do[:, h * hd:(h + 1) * hd]
        qs_ref[h * ROWS:(h + 1) * ROWS] = q[:, h * hd:(h + 1) * hd]
        dot_ref[:, h * ROWS:(h + 1) * ROWS] = do[:, h * hd:(h + 1) * hd].T
    delta = jnp.sum(dot_ref[...].astype(jnp.float32) * ot_ref[0].astype(jnp.float32), axis=0, keepdims=True)
    inv = li_ref[0]
    dqt_ref[...] = jnp.zeros_like(dqt_ref)

    def body(blk, carry):
        k_b = k_ref[blk].reshape(n_chunks * ROWS, hd)
        v_b = v_ref[blk].reshape(n_chunks * ROWS, hd)
        s = jnp.dot(k_b, qt_ref[0], preferred_element_type=jnp.float32)
        dp = jnp.dot(v_b, dot_ref[...], preferred_element_type=jnp.float32)
        t = jnp.tanh(s * (1.0 / SOFT_CAP))
        p = masked_exp(t, key_mask(posq_ref, posk_ref, blk), n_heads) * inv
        ds = (p * (dp - delta) * (1.0 - t * t)).astype(jnp.bfloat16)
        dv_ref[blk] += jnp.dot(p.astype(jnp.bfloat16), dos_ref[...], preferred_element_type=jnp.float32)
        dk_ref[blk] += jnp.dot(ds, qs_ref[...], preferred_element_type=jnp.float32)
        kt = jnp.concatenate([kt_ref[blk, c] for c in range(n_chunks)], axis=1)
        dqt_ref[...] += jnp.dot(kt, ds, preferred_element_type=jnp.float32)
        return carry

    lax.fori_loop(lo_ref[own], own + 1, body, 0)

    def unrope(grad, cos, sin):
        lo, hi = grad[:, :half], grad[:, half:]
        return lo * cos + hi * sin, hi * cos - lo * sin

    cos, sin = cos_ref[own, chunk], sin_ref[own, chunk]
    for h in range(n_heads):
        lo, hi = unrope(dqt_ref[:, h * ROWS:(h + 1) * ROWS].T, cos, sin)
        dq_ref[0, :, h * hd:h * hd + half] = (lo * scale).astype(jnp.bfloat16)
        dq_ref[0, :, h * hd + half:(h + 1) * hd] = (hi * scale).astype(jnp.bfloat16)

    if last:
        @pl.when(own == n_own - 1)
        def _():
            def fin(i, carry):
                for c in range(n_chunks):
                    lo, hi = unrope(dk_ref[i, c * ROWS:(c + 1) * ROWS], cos_ref[i, c], sin_ref[i, c])
                    dk_out[i, c, :, :half] = lo.astype(jnp.bfloat16)
                    dk_out[i, c, :, half:] = hi.astype(jnp.bfloat16)
                    dv_out[i, c] = dv_ref[i, c * ROWS:(c + 1) * ROWS].astype(jnp.bfloat16)
                return carry
            lax.fori_loop(0, n_own, fin, 0)


def attn_bwd(n_heads, scale, chunk, first, last, lo, q, qt, ot, li, do, k, kt, v, posq, posk, cos_t, sin_t, prev):
    n_own, n_chunks, rows, hd = k.shape
    lanes = n_heads * rows
    full = lambda x: pl.BlockSpec(x.shape, lambda i, lo: (0,) * x.ndim)
    per = lambda s: pl.BlockSpec((1,) + s, lambda i, lo: (i, 0, 0))
    acc = jax.ShapeDtypeStruct((n_own, n_chunks * rows, hd), jnp.float32)
    fin = jax.ShapeDtypeStruct((n_own, n_chunks, rows, hd), jnp.bfloat16)
    kv_out = fin if last else acc
    scratch = [pltpu.VMEM(acc.shape, jnp.float32)] * 2 if last else []
    scratch += [pltpu.VMEM((hd, lanes), jnp.float32), pltpu.VMEM((hd, lanes), jnp.bfloat16),
                pltpu.VMEM((lanes, hd), jnp.bfloat16), pltpu.VMEM((lanes, hd), jnp.bfloat16)]
    return pl.pallas_call(
        functools.partial(bwd_kernel, n_heads, scale, chunk, first, last),
        grid_spec=pltpu.PrefetchScalarGridSpec(
            num_scalar_prefetch=1, grid=(n_own,),
            in_specs=[pl.BlockSpec((1, 1, rows, n_heads * hd), lambda i, lo: (i, chunk, 0, 0)), per((hd, lanes)), per((hd, lanes)), per((1, lanes)),
                      per((rows, n_heads * hd)), full(k), full(kt), full(v), per((1, rows)), full(posk),
                      full(cos_t), full(sin_t)] + [full(x) for x in prev],
            out_specs=[per((rows, n_heads * hd)), full(kv_out), full(kv_out)],
            scratch_shapes=scratch),
        out_shape=[jax.ShapeDtypeStruct((n_own, rows, n_heads * hd), jnp.bfloat16), kv_out, kv_out],
        compiler_params=params(),
        cost_estimate=pl.CostEstimate(flops=10 * n_own * lanes * (n_own * n_chunks * rows // 2) * hd,
                                      transcendentals=0, bytes_accessed=24 * k.size),
        name="attn_bwd",
    )(lo, q, qt, ot, li, do, k, kt, v, posq, posk, cos_t, sin_t, *prev)


def matmul(lhs, rhs, dims):
    return lax.dot_general(lhs, rhs, (dims, ((), ())), preferred_element_type=jnp.float32)


def solution(mesh):
    act_spec = P('dp', 'tp', None)
    head_spec = P(None, 'tp', None)
    grad_spec = P('dp', 'tp', None)
    in_specs = (act_spec, P('dp', 'tp'), act_spec, head_spec, head_spec, head_spec, P('tp', None, None), P(None), P(None))
    out_specs = (act_spec, act_spec, grad_spec, grad_spec, grad_spec, P(('dp', 'tp'), None, None), P('dp'), P('dp'))
    n_own = mesh.shape['tp']

    def local_step(x_in, positions, grad_out, w_query, w_key, w_value, w_out, gain_pre, gain_post):
        d_model, n_heads, hd = w_query.shape
        loc = x_in.shape[1]
        n_chunks = loc // ROWS
        scale = hd ** -0.5
        half = hd // 2
        qw = n_heads * hd
        chunks = range(n_chunks)
        x_c = [x_in[0, c * ROWS:(c + 1) * ROWS] for c in chunks]
        g_c = [grad_out[0, c * ROWS:(c + 1) * ROWS] for c in chunks]
        w_cat = jnp.concatenate([w_query.reshape(d_model, qw), w_key.reshape(d_model, hd), w_value.reshape(d_model, hd)], axis=1)
        wo = w_out.reshape(qw, d_model)

        normed, pre_pullback = jax.vjp(rms_norm, x_in[0], gain_pre)
        a_all = lax.all_gather(normed, 'tp', axis=0, tiled=True)
        pos = lax.all_gather(positions, 'tp', axis=1, tiled=True).reshape(n_own, n_chunks, ROWS)
        inv_freq = ROPE_THETA ** (-2.0 * jnp.arange(half, dtype=jnp.float32) / hd)
        angles = pos.astype(jnp.float32)[..., None] * inv_freq
        cos_t, sin_t = jnp.cos(angles), jnp.sin(angles)
        pos_k = jnp.broadcast_to(pos.reshape(n_own, loc, 1), (n_own, loc, ROWS))
        k_last = pos[:, -1, -1]
        lo = jnp.sum((pos[:, :, :1] - k_last >= WINDOW).astype(jnp.int32), axis=-1)
        pos_q = [pos[:, c:c + 1] for c in chunks]
        lo_c = [lo[:, c] for c in chunks]

        q_all, k_all, kt_all, v_all, vt_all = qkv(n_heads, scale, a_all.reshape(n_own, n_chunks, ROWS, d_model), w_cat, cos_t, sin_t)

        saved, r_c = [], []
        for c in chunks:
            o, ot, qt, li = attn_fwd(n_heads, c, lo_c[c], q_all, k_all, vt_all, pos_q[c], pos_k)
            saved.append((o, ot, qt, li))
            part = matmul(o.reshape(n_own * ROWS, qw), wo, ((1,), (0,))).astype(jnp.bfloat16)
            r_c.append(lax.psum_scatter(part, 'tp', scatter_dimension=0, tiled=True))

        y_c, dp_c, d_gain_post = [], [], 0.0
        for c in chunks:
            post, pullback = jax.vjp(rms_norm, r_c[c], gain_post)
            y_c.append((x_c[c].astype(jnp.float32) + post.astype(jnp.float32)).astype(jnp.bfloat16))
            d_proj, d_gain = pullback(g_c[c])
            d_gain_post = d_gain_post + d_gain
            dp_c.append(lax.all_gather(d_proj, 'tp', axis=0, tiled=True))

        dq_c, dkv = [], ()
        for c in chunks:
            o, ot, qt, li = saved[c]
            do = matmul(dp_c[c], wo, ((1,), (1,))).astype(jnp.bfloat16).reshape(n_own, ROWS, qw)
            dq, *dkv = attn_bwd(n_heads, scale, c, c == 0, c == n_chunks - 1, lo_c[c], q_all, qt, ot, li, do,
                                k_all, kt_all, v_all, pos_q[c], pos_k, cos_t, sin_t, dkv)
            dq_c.append(dq)
        dk_all, dv_all = dkv

        dcat = jnp.concatenate([jnp.stack(dq_c, axis=1), dk_all, dv_all], axis=-1)
        da_c = []
        for c in chunks:
            part = matmul(dcat[:, c].reshape(n_own * ROWS, qw + 2 * hd), w_cat, ((1,), (1,))).astype(jnp.bfloat16)
            da_c.append(lax.psum_scatter(part, 'tp', scatter_dimension=0, tiled=True))
        grad_wo = sum(matmul(saved[c][0].reshape(n_own * ROWS, qw), dp_c[c], ((0,), (0,))) for c in chunks).reshape(n_heads, hd, d_model)
        g_cat = matmul(a_all, dcat.reshape(n_own * loc, qw + 2 * hd), ((0,), (0,)))
        grad_wq = g_cat[:, :qw].reshape(d_model, n_heads, hd)
        grad_wk = g_cat[:, qw:qw + hd].reshape(d_model, 1, hd)
        grad_wv = g_cat[:, qw + hd:].reshape(d_model, 1, hd)

        d_x, d_gain_pre = pre_pullback(jnp.concatenate(da_c, axis=0))
        grad_x = (grad_out.astype(jnp.float32) + d_x.astype(jnp.float32)).astype(jnp.bfloat16)
        grad_pre = lax.psum(d_gain_pre, 'tp')
        grad_post = lax.psum(d_gain_post, 'tp')
        y_out = jnp.concatenate(y_c, axis=0)[None]
        return y_out, grad_x, grad_wq, grad_wk, grad_wv, grad_wo, grad_pre, grad_post

    return jax.shard_map(local_step, mesh=mesh, in_specs=in_specs, out_specs=out_specs, check_vma=False)
```

```python
import functools

import jax
import jax.numpy as jnp
from jax import lax
from jax.experimental import pallas as pl
from jax.experimental.pallas import tpu as pltpu
from jax.sharding import PartitionSpec as P

WINDOW = 4096
SOFT_CAP = 50.0
NORM_EPS = 1e-6
ROPE_THETA = 10000.0
ROWS = 128
LOG2E = 1.4426950408889634
VMEM_LIMIT = 60 * 1024 * 1024
KEY_BLOCKS = 3


def rms_norm(hidden, scale_w):
    values = hidden.astype(jnp.float32)
    inv_rms = lax.rsqrt(jnp.mean(values * values, axis=-1, keepdims=True) + NORM_EPS)
    return (values * inv_rms * (1.0 + scale_w)).astype(jnp.bfloat16)


def params(n=1):
    return pltpu.CompilerParams(dimension_semantics=("arbitrary",) * n, vmem_limit_bytes=VMEM_LIMIT)


def key_mask(posq_ref, posk_ref, start, limit):
    keys = KEY_BLOCKS * ROWS
    gap = posq_ref[0, 0] - posk_ref[pl.ds(start, KEY_BLOCKS)].reshape(keys, ROWS)
    row = lax.broadcasted_iota(jnp.int32, (keys, ROWS), 0)
    return (gap >= 0) & (gap < WINDOW) & (row < limit)


def key_range(lo_ref, own, cur, n_chunks):
    end = own * n_chunks + cur + 1
    steps = (end - lo_ref[end - 1] + KEY_BLOCKS - 1) // KEY_BLOCKS

    def at(i):
        stop = end - KEY_BLOCKS * i
        start = jnp.maximum(stop - KEY_BLOCKS, 0)
        return start, (stop - start) * ROWS

    return steps, at


def side_by_side(ref, start):
    return jnp.concatenate([ref[start + c] for c in range(KEY_BLOCKS)], axis=1)


def masked_exp(t, mask, n_heads):
    e = jnp.exp2(t * (SOFT_CAP * LOG2E))
    return jnp.concatenate([jnp.where(mask, e[:, h * ROWS:(h + 1) * ROWS], 0.0) for h in range(n_heads)], axis=1)


def fwd_kernel(n_heads, lo_ref, q_ref, k_ref, vt_ref, posq_ref, posk_ref, o_ref, ot_ref, qt_ref, li_ref, acc_ref):
    own, cur = pl.program_id(0), pl.program_id(1)
    n_chunks, hd = pl.num_programs(1), k_ref.shape[2]
    keys = KEY_BLOCKS * ROWS
    q = q_ref[0, 0]
    qt = jnp.concatenate([q[:, h * hd:(h + 1) * hd].T for h in range(n_heads)], axis=1)
    qt_ref[0, 0] = qt
    acc_ref[...] = jnp.zeros_like(acc_ref)

    steps, at = key_range(lo_ref, own, cur, n_chunks)

    def body(i, l_sum):
        start, limit = at(i)
        k_b = k_ref[pl.ds(start, KEY_BLOCKS)].reshape(keys, hd)
        s = jnp.dot(k_b, qt_ref[0, 0], preferred_element_type=jnp.float32)
        t = jnp.tanh(s * (1.0 / SOFT_CAP))
        e = masked_exp(t, key_mask(posq_ref, posk_ref, start, limit), n_heads)
        acc_ref[...] += jnp.dot(side_by_side(vt_ref, start), e.astype(jnp.bfloat16), preferred_element_type=jnp.float32)
        return l_sum + jnp.sum(e, axis=0, keepdims=True)

    l_sum = lax.fori_loop(0, steps, body, jnp.zeros((1, n_heads * ROWS), jnp.float32))
    inv = 1.0 / l_sum
    li_ref[0, 0] = inv
    ot = (acc_ref[...] * inv).astype(jnp.bfloat16)
    ot_ref[0, 0] = ot
    for h in range(n_heads):
        o_ref[0, 0, :, h * hd:(h + 1) * hd] = ot[:, h * ROWS:(h + 1) * ROWS].T


def attn_fwd(n_heads, lo, q, k, vt, posq, posk):
    n_own, n_chunks, rows = q.shape[:3]
    hd = k.shape[-1]
    lanes = n_heads * rows
    full = lambda x: pl.BlockSpec(x.shape, lambda i, c, lo: (0,) * x.ndim)
    per = lambda s: pl.BlockSpec((1, 1) + s, lambda i, c, lo: (i, c, 0, 0))
    out = lambda s, t: jax.ShapeDtypeStruct((n_own, n_chunks) + s, t)
    return pl.pallas_call(
        functools.partial(fwd_kernel, n_heads),
        grid_spec=pltpu.PrefetchScalarGridSpec(
            num_scalar_prefetch=1, grid=(n_own, n_chunks),
            in_specs=[per((rows, n_heads * hd)), full(k), full(vt), per((1, rows)), full(posk)],
            out_specs=[per((rows, n_heads * hd)), per((hd, lanes)), per((hd, lanes)), per((1, lanes))],
            scratch_shapes=[pltpu.VMEM((hd, lanes), jnp.float32)]),
        out_shape=[out((rows, n_heads * hd), jnp.bfloat16), out((hd, lanes), jnp.bfloat16),
                   out((hd, lanes), jnp.bfloat16), out((1, lanes), jnp.float32)],
        compiler_params=params(2),
        cost_estimate=pl.CostEstimate(flops=2 * q.size * n_own * n_chunks * rows, transcendentals=0, bytes_accessed=12 * k.size),
        name="attn_fwd",
    )(lo, q, k, vt, posq, posk)


def bwd_kernel(n_heads, scale, lo_ref, q_ref, qt_ref, ot_ref, li_ref, do_ref, k_ref, kt_ref, v_ref, posq_ref, posk_ref,
               cos_ref, sin_ref, out_ref, dk_ref, dv_ref, dqt_ref, dot_ref, dos_ref, qs_ref):
    own, cur = pl.program_id(0), pl.program_id(1)
    n_own, n_chunks, hd = pl.num_programs(0), pl.num_programs(1), k_ref.shape[2]
    keys = KEY_BLOCKS * ROWS
    half = hd // 2
    qw = n_heads * hd

    @pl.when((own == 0) & (cur == 0))
    def _():
        dk_ref[...] = jnp.zeros_like(dk_ref)
        dv_ref[...] = jnp.zeros_like(dv_ref)

    do = do_ref[0, 0]
    q = q_ref[0, 0]
    for h in range(n_heads):
        dos_ref[h * ROWS:(h + 1) * ROWS] = do[:, h * hd:(h + 1) * hd]
        qs_ref[h * ROWS:(h + 1) * ROWS] = q[:, h * hd:(h + 1) * hd]
        dot_ref[:, h * ROWS:(h + 1) * ROWS] = do[:, h * hd:(h + 1) * hd].T
    delta = jnp.sum(dot_ref[...].astype(jnp.float32) * ot_ref[0, 0].astype(jnp.float32), axis=0, keepdims=True)
    inv = li_ref[0, 0]
    dqt_ref[...] = jnp.zeros_like(dqt_ref)

    steps, at = key_range(lo_ref, own, cur, n_chunks)

    def body(i, carry):
        start, limit = at(i)
        here = pl.ds(start, KEY_BLOCKS)
        k_b = k_ref[here].reshape(keys, hd)
        v_b = v_ref[here].reshape(keys, hd)
        s = jnp.dot(k_b, qt_ref[0, 0], preferred_element_type=jnp.float32)
        dp = jnp.dot(v_b, dot_ref[...], preferred_element_type=jnp.float32)
        t = jnp.tanh(s * (1.0 / SOFT_CAP))
        p = masked_exp(t, key_mask(posq_ref, posk_ref, start, limit), n_heads) * inv
        ds = (p * (dp - delta) * (1.0 - t * t)).astype(jnp.bfloat16)
        dv_ref[here] += jnp.dot(p.astype(jnp.bfloat16), dos_ref[...], preferred_element_type=jnp.float32).reshape(KEY_BLOCKS, ROWS, hd)
        dk_ref[here] += jnp.dot(ds, qs_ref[...], preferred_element_type=jnp.float32).reshape(KEY_BLOCKS, ROWS, hd)
        dqt_ref[...] += jnp.dot(side_by_side(kt_ref, start), ds, preferred_element_type=jnp.float32)
        return carry

    lax.fori_loop(0, steps, body, 0)

    def unrope(grad, cos, sin):
        lo, hi = grad[:, :half], grad[:, half:]
        return lo * cos + hi * sin, hi * cos - lo * sin

    cos, sin = cos_ref[own, cur], sin_ref[own, cur]
    for h in range(n_heads):
        lo, hi = unrope(dqt_ref[:, h * ROWS:(h + 1) * ROWS].T, cos, sin)
        out_ref[own, cur, :, h * hd:h * hd + half] = (lo * scale).astype(jnp.bfloat16)
        out_ref[own, cur, :, h * hd + half:(h + 1) * hd] = (hi * scale).astype(jnp.bfloat16)

    @pl.when((own == n_own - 1) & (cur == n_chunks - 1))
    def _():
        def fin(i, carry):
            for c in range(out_ref.shape[1]):
                b = i * out_ref.shape[1] + c
                lo, hi = unrope(dk_ref[b], cos_ref[i, c], sin_ref[i, c])
                out_ref[i, c, :, qw:qw + half] = lo.astype(jnp.bfloat16)
                out_ref[i, c, :, qw + half:qw + hd] = hi.astype(jnp.bfloat16)
                out_ref[i, c, :, qw + hd:] = dv_ref[b].astype(jnp.bfloat16)
            return carry
        lax.fori_loop(0, n_own, fin, 0)


def attn_bwd(n_heads, scale, lo, q, qt, ot, li, do, k, kt, v, posq, posk, cos_t, sin_t):
    n_own, n_chunks, rows = q.shape[:3]
    hd = k.shape[-1]
    lanes = n_heads * rows
    once = dict(pipeline_mode=pl.Buffered(1))
    full = lambda x: pl.BlockSpec(x.shape, lambda i, c, lo: (0,) * x.ndim, **once)
    per = lambda s: pl.BlockSpec((1, 1) + s, lambda i, c, lo: (i, c, 0, 0))
    out = jax.ShapeDtypeStruct((n_own, n_chunks, rows, (n_heads + 2) * hd), jnp.bfloat16)
    acc = pltpu.VMEM(k.shape, jnp.float32)
    return pl.pallas_call(
        functools.partial(bwd_kernel, n_heads, scale),
        grid_spec=pltpu.PrefetchScalarGridSpec(
            num_scalar_prefetch=1, grid=(n_own, n_chunks),
            in_specs=[per((rows, n_heads * hd)), per((hd, lanes)), per((hd, lanes)), per((1, lanes)),
                      per((rows, n_heads * hd)), full(k), full(kt), full(v), per((1, rows)), full(posk),
                      full(cos_t), full(sin_t)],
            out_specs=pl.BlockSpec(out.shape, lambda i, c, lo: (0, 0, 0, 0)),
            scratch_shapes=[acc, acc, pltpu.VMEM((hd, lanes), jnp.float32), pltpu.VMEM((hd, lanes), jnp.bfloat16),
                            pltpu.VMEM((lanes, hd), jnp.bfloat16), pltpu.VMEM((lanes, hd), jnp.bfloat16)]),
        out_shape=out,
        compiler_params=params(2),
        cost_estimate=pl.CostEstimate(flops=5 * q.size * n_own * n_chunks * rows, transcendentals=0, bytes_accessed=24 * k.size),
        name="attn_bwd",
    )(lo, q, qt, ot, li, do, k, kt, v, posq, posk, cos_t, sin_t)


MESH = pl.DeviceIdType.MESH


def ring_ids(n):
    me = lax.axis_index('tp')
    return me, me + 1 - 2 * (me % 2), (me + 2) % n, (me + n - 2) % n


def greet(peers):
    barrier = pltpu.get_barrier_semaphore()
    for peer in peers:
        pl.semaphore_signal(barrier, inc=1, device_id={'tp': peer}, device_id_type=MESH)
    pl.semaphore_wait(barrier, len(peers))


def comm_params(cid):
    return pltpu.CompilerParams(collective_id=cid, has_side_effects=True, vmem_limit_bytes=63 * 1024 * 1024)


def gather_ring(n, src_ref, all_ref, send, recv, compute):
    me, partner, right, left = ring_ids(n)
    opp = (me + n // 2) % n
    half = src_ref.shape[0] // 2

    def part(owner, h):
        return all_ref.at[owner, pl.ds(h * half, half)]

    def copy(idx, src, owner, h, target):
        return pltpu.make_async_remote_copy(src_ref=src, dst_ref=part(owner, h), send_sem=send.at[idx], recv_sem=recv.at[idx],
                                            device_id={'tp': target}, device_id_type=MESH)

    def own(idx, h, target):
        return copy(idx, src_ref.at[pl.ds(h * half, half)], me, h, target)

    def fwd(idx, owner, h, target):
        return copy(idx, part(owner, h), owner, h, target)

    def arrived(idx, owner, h):
        fwd(idx, owner, h, partner).wait_recv()

    firsts = [own(0, 0, right), own(2, 1, left), own(1, 1, right), own(3, 0, left), own(4, 0, partner), own(5, 1, partner)]
    for c in firsts:
        c.start()
    all_ref[me] = src_ref[...]
    relays = [fwd(6, left, 0, right), fwd(7, right, 1, left), fwd(8, left, 0, partner), fwd(9, left, 1, partner),
              fwd(10, right, 1, partner), fwd(11, right, 0, partner), fwd(12, opp, 0, partner), fwd(13, opp, 1, partner)]
    l_par, r_par, o_par = (partner + n - 2) % n, (partner + 2) % n, (partner + n // 2) % n
    order = (me, partner, left, right, l_par, r_par, opp, o_par)

    def step(i, carry):
        @pl.when(i == 1)
        def _():
            arrived(4, partner, 0)
            arrived(5, partner, 1)

        @pl.when(i == 2)
        def _():
            arrived(0, left, 0)
            relays[0].start()
            relays[2].start()
            arrived(2, right, 1)
            relays[1].start()
            relays[4].start()
            arrived(1, left, 1)
            relays[3].start()

        @pl.when(i == 3)
        def _():
            arrived(3, right, 0)
            relays[5].start()

        @pl.when(i == 4)
        def _():
            arrived(8, l_par, 0)
            arrived(9, l_par, 1)

        @pl.when(i == 5)
        def _():
            arrived(10, r_par, 1)
            arrived(11, r_par, 0)

        @pl.when(i == 6)
        def _():
            arrived(6, opp, 0)
            relays[6].start()
            arrived(7, opp, 1)
            relays[7].start()

        @pl.when(i == 7)
        def _():
            arrived(12, o_par, 0)
            arrived(13, o_par, 1)

        owner = order[0]
        for j in range(1, len(order)):
            owner = jnp.where(i == j, order[j], owner)
        compute(owner)
        return carry

    lax.fori_loop(0, n, step, 0)
    for c in firsts + relays:
        c.wait_send()


def gather_scratch(n, rows, d_model):
    return [pltpu.VMEM((n, rows, d_model), jnp.bfloat16), pltpu.SemaphoreType.DMA((14,)), pltpu.SemaphoreType.DMA((14,))]


def qkv_kernel(n, n_heads, scale, x_ref, gain_ref, w_ref, cos_ref, sin_ref, a_ref, q_ref, k_ref, kt_ref, v_ref, vt_ref,
               own_ref, all_ref, send, recv, out_sem):
    rows = x_ref.shape[0]
    n_chunks, half = cos_ref.shape[1], cos_ref.shape[3]
    hd = 2 * half
    own_ref[...] = rms_norm(x_ref[...], gain_ref[...])
    _, partner, right, left = ring_ids(n)
    greet((partner, right, left))

    def to_hbm(owner):
        return pltpu.make_async_copy(all_ref.at[owner], a_ref.at[owner], out_sem.at[owner])

    def compute(owner):
        to_hbm(owner).start()
        lin = jnp.dot(all_ref[owner], w_ref[...], preferred_element_type=jnp.float32)
        cos = cos_ref[owner].reshape(rows, half)
        sin = sin_ref[owner].reshape(rows, half)

        def rope(col):
            lo = lin[:, col:col + half]
            hi = lin[:, col + half:col + hd]
            return lo * cos - hi * sin, hi * cos + lo * sin

        for h in range(n_heads):
            lo, hi = rope(h * hd)
            q_ref[owner, :, :, h * hd:h * hd + half] = (lo * scale).astype(jnp.bfloat16).reshape(n_chunks, ROWS, half)
            q_ref[owner, :, :, h * hd + half:(h + 1) * hd] = (hi * scale).astype(jnp.bfloat16).reshape(n_chunks, ROWS, half)
        lo, hi = rope(n_heads * hd)
        k = jnp.concatenate([lo.astype(jnp.bfloat16), hi.astype(jnp.bfloat16)], axis=1)
        v = lin[:, (n_heads + 1) * hd:].astype(jnp.bfloat16)
        for c in range(n_chunks):
            b = owner * n_chunks + c
            k_c = k[c * ROWS:(c + 1) * ROWS]
            v_c = v[c * ROWS:(c + 1) * ROWS]
            k_ref[b] = k_c
            kt_ref[b] = k_c.T
            v_ref[b] = v_c
            vt_ref[b] = v_c.T

    gather_ring(n, own_ref, all_ref, send, recv, compute)

    def drain(i, carry):
        to_hbm(i).wait()
        return carry

    lax.fori_loop(0, n, drain, 0)


def gather_qkv(n, n_heads, scale, x, gain, w, cos_t, sin_t):
    rows, d_model = x.shape
    n_chunks, hd = cos_t.shape[1], 2 * cos_t.shape[3]
    blocks = n * n_chunks
    bf = lambda s: jax.ShapeDtypeStruct(s, jnp.bfloat16)
    vmem = pl.BlockSpec(memory_space=pltpu.VMEM)
    return pl.pallas_call(
        functools.partial(qkv_kernel, n, n_heads, scale),
        in_specs=[vmem] * 5, out_specs=[pl.BlockSpec(memory_space=pl.ANY)] + [vmem] * 5,
        out_shape=[bf((n, rows, d_model)), bf((n, n_chunks, ROWS, n_heads * hd)),
                   bf((blocks, ROWS, hd)), bf((blocks, hd, ROWS)), bf((blocks, ROWS, hd)), bf((blocks, hd, ROWS))],
        scratch_shapes=[pltpu.VMEM((rows, d_model), jnp.bfloat16)] + gather_scratch(n, rows, d_model) + [pltpu.SemaphoreType.DMA((n,))],
        compiler_params=comm_params(0),
        cost_estimate=pl.CostEstimate(flops=2 * n * x.size * w.shape[1], transcendentals=0, bytes_accessed=4 * n * x.size),
        name="gather_qkv",
    )(x, gain, w, cos_t, sin_t)


def dproj_kernel(n, n_heads, x_ref, wo_ref, ot_ref, do_ref, gwo_ref, all_ref, send, recv):
    n_chunks, hd = ot_ref.shape[1], ot_ref.shape[2]
    _, partner, right, left = ring_ids(n)
    greet((partner, right, left))
    gwo_ref[...] = jnp.zeros_like(gwo_ref)

    def compute(owner):
        dp = all_ref[owner]
        do = lax.dot_general(dp, wo_ref[...], (((1,), (1,)), ((), ())), preferred_element_type=jnp.float32)
        do_ref[owner] = do.astype(jnp.bfloat16).reshape(n_chunks, ROWS, n_heads * hd)
        for h in range(n_heads):
            ot = jnp.concatenate([ot_ref[owner, c, :, h * ROWS:(h + 1) * ROWS] for c in range(n_chunks)], axis=1)
            gwo_ref[h * hd:(h + 1) * hd] += jnp.dot(ot, dp, preferred_element_type=jnp.float32)

    gather_ring(n, x_ref, all_ref, send, recv, compute)


def gather_dproj(n, n_heads, d_proj, wo, ot):
    rows, d_model = d_proj.shape
    n_chunks, hd = ot.shape[1], ot.shape[2]
    vmem = pl.BlockSpec(memory_space=pltpu.VMEM)
    return pl.pallas_call(
        functools.partial(dproj_kernel, n, n_heads),
        in_specs=[vmem] * 3, out_specs=[vmem] * 2,
        out_shape=[jax.ShapeDtypeStruct((n, n_chunks, ROWS, n_heads * hd), jnp.bfloat16),
                   jax.ShapeDtypeStruct((n_heads * hd, d_model), jnp.float32)],
        scratch_shapes=gather_scratch(n, rows, d_model),
        compiler_params=comm_params(1),
        cost_estimate=pl.CostEstimate(flops=4 * n * rows * d_model * n_heads * hd, transcendentals=0, bytes_accessed=2 * n * d_proj.size),
        name="gather_dproj",
    )(d_proj, wo, ot)


def scatter_kernel(n, trans, pieces, n_heads, *refs):
    if n_heads:
        lhs_ref, rhs_ref, a_ref, out_ref, gq_ref, gk_ref, gv_ref = refs[:7]
        a_buf, g_bufs, a_sem, g_sem = refs[-6], refs[-5:-2], refs[-2], refs[-1]
        acc, pst, pin, rcv, p_send, p_recv, r_send, r_recv = refs[7:-6]
    else:
        lhs_ref, rhs_ref, out_ref, acc, pst, pin, rcv, p_send, p_recv, r_send, r_recv = refs
    me, partner, right, left = ring_ids(n)
    core = me % 2
    chips = n // 2
    chip = me // 2
    width = acc.shape[2]
    rows = acc.shape[1]
    prow = rows // pieces
    hop = (right, left)
    greet((partner, right, left))

    if n_heads:
        tile = a_buf.shape[2]
        hd = gk_ref.shape[2]
        tiles = a_ref.shape[1] // tile
        per_stage = tiles // (chips - 1)
        depth = lhs_ref.shape[2]

        def a_in(t):
            return pltpu.make_async_copy(a_ref.at[:, pl.ds(pl.multiple_of(t * tile, tile), tile)], a_buf.at[t % 2], a_sem.at[t % 2])

        def g_out(t):
            at = pl.ds(pl.multiple_of(t * tile, tile), tile)
            return [pltpu.make_async_copy(b.at[t % 2], g.at[at], g_sem.at[t % 2, i])
                    for i, (b, g) in enumerate(zip(g_bufs, (gq_ref, gk_ref, gv_ref)))]

        def wgrad(t, carry):
            a_in(t).wait()

            @pl.when(t + 1 < tiles)
            def _():
                a_in(t + 1).start()

            @pl.when(t >= 2)
            def _():
                for c in g_out(t - 2):
                    c.wait()

            g = lax.dot_general(a_buf[t % 2], lhs_ref[...].reshape(n * rows, depth), (((0,), (0,)), ((), ())),
                                preferred_element_type=jnp.float32)
            for h in range(n_heads):
                g_bufs[0][t % 2, :, h, :] = g[:, h * hd:(h + 1) * hd]
            g_bufs[1][t % 2, :, 0, :] = g[:, n_heads * hd:(n_heads + 1) * hd]
            g_bufs[2][t % 2, :, 0, :] = g[:, (n_heads + 1) * hd:]
            for c in g_out(t):
                c.start()
            return carry

        a_in(0).start()

    def partial_sum(owner, d):
        if trans:
            return lax.dot_general(lhs_ref[owner], rhs_ref[d * width:(d + 1) * width], (((1,), (1,)), ((), ())),
                                   preferred_element_type=jnp.float32)
        return jnp.dot(lhs_ref[owner], rhs_ref[:, d * width:(d + 1) * width], preferred_element_type=jnp.float32)

    def to_partner(j, d):
        return pltpu.make_async_remote_copy(src_ref=pst.at[j % 2, d], dst_ref=pin.at[j, d], send_sem=p_send.at[j, d],
                                            recv_sem=p_recv.at[j, d], device_id={'tp': partner}, device_id_type=MESH)

    def to_next(j, d, p):
        at = pl.ds(p * prow, prow)
        return pltpu.make_async_remote_copy(src_ref=pin.at[j, d, at], dst_ref=rcv.at[j, d, at], send_sem=r_send.at[j, d, p],
                                            recv_sem=r_recv.at[j, d, p], device_id={'tp': hop[d]}, device_id_type=MESH)

    def stage(j, carry):
        dest = ((chip + 2 * chips - 1 - j) % chips, (chip + 1 + j) % chips)

        @pl.when(j >= 2)
        def _():
            for d in range(2):
                to_partner(j - 2, d).wait_send()

        for d in range(2):
            pst[j % 2, d] = partial_sum(dest[d] * 2 + 1 - core, d).astype(jnp.bfloat16)
            to_partner(j, d).start()
        for d in range(2):
            acc[d] = partial_sum(dest[d] * 2 + core, d)
        for d in range(2):
            to_partner(j, d).wait_recv()
        for p in range(pieces):
            at = slice(p * prow, (p + 1) * prow)
            for d in range(2):
                @pl.when(j == 0)
                def _():
                    pin[0, d, at] = (acc[d, at] + pin[0, d, at].astype(jnp.float32)).astype(jnp.bfloat16)
                    to_next(0, d, p).start()

                @pl.when((j > 0) & (j < chips - 1))
                def _():
                    to_next(j - 1, d, p).wait_recv()
                    pin[j, d, at] = (acc[d, at] + pin[j, d, at].astype(jnp.float32)
                                     + rcv[j - 1, d, at].astype(jnp.float32)).astype(jnp.bfloat16)
                    to_next(j, d, p).start()

                @pl.when(j == chips - 1)
                def _():
                    to_next(chips - 2, d, p).wait_recv()
                    out_ref[at, d * width:(d + 1) * width] = (
                        acc[d, at] + pin[chips - 1, d, at].astype(jnp.float32)
                        + rcv[chips - 2, d, at].astype(jnp.float32)).astype(jnp.bfloat16)
        if n_heads:
            first = jnp.minimum(j * per_stage, tiles)
            lax.fori_loop(first, jnp.minimum(first + per_stage, tiles), wgrad, 0)
        return carry

    lax.fori_loop(0, chips, stage, 0)
    if n_heads:
        for t in (tiles - 2, tiles - 1):
            for c in g_out(t):
                c.wait()
    for d in range(2):
        for j in (chips - 2, chips - 1):
            to_partner(j, d).wait_send()
        for j in range(chips - 1):
            for p in range(pieces):
                to_next(j, d, p).wait_send()


def matmul_scatter(n, cid, trans, lhs, rhs, a=None, n_heads=0):
    rows, depth = lhs.shape[1:]
    d_model = rhs.shape[0] if trans else rhs.shape[1]
    chips, width, pieces = n // 2, d_model // 2, 3
    vmem = pl.BlockSpec(memory_space=pltpu.VMEM)
    hbm = pl.BlockSpec(memory_space=pl.ANY)
    bf = lambda k: pltpu.VMEM((k, 2, rows, width), jnp.bfloat16)
    dma = pltpu.SemaphoreType.DMA
    out_shape = [jax.ShapeDtypeStruct((rows, d_model), jnp.bfloat16)]
    scratch = [pltpu.VMEM((2, rows, width), jnp.float32), bf(2), bf(chips), bf(chips - 1),
               dma((chips, 2)), dma((chips, 2)), dma((chips - 1, 2, pieces)), dma((chips - 1, 2, pieces))]
    args = [lhs, rhs]
    flops = 2 * n * rows * depth * d_model
    if n_heads:
        hd, tile = depth // (n_heads + 2), 256
        args.append(a)
        out_shape += [jax.ShapeDtypeStruct((d_model, k, hd), jnp.float32) for k in (n_heads, 1, 1)]
        scratch += [pltpu.VMEM((2, n * rows, tile), jnp.bfloat16)]
        scratch += [pltpu.VMEM((2, tile, k, hd), jnp.float32) for k in (n_heads, 1, 1)] + [dma((2,)), dma((2, 3))]
        flops *= 2
    return pl.pallas_call(
        functools.partial(scatter_kernel, n, trans, pieces, n_heads),
        in_specs=[vmem] * 2 + [hbm] * (len(args) - 2), out_specs=[vmem] + [hbm] * (len(out_shape) - 1),
        out_shape=out_shape,
        scratch_shapes=scratch,
        compiler_params=comm_params(cid),
        cost_estimate=pl.CostEstimate(flops=flops, transcendentals=0, bytes_accessed=2 * n * rows * d_model),
        name="matmul_scatter",
    )(*args)


def total_kernel(n, x_ref, out_ref, buf, send, recv):
    me = lax.axis_index('tp')
    peers = [(me + i) % n for i in range(1, n)]
    greet(peers)
    out = [pltpu.make_async_remote_copy(src_ref=x_ref, dst_ref=buf.at[me], send_sem=send.at[i], recv_sem=recv.at[i],
                                        device_id={'tp': peers[i]}, device_id_type=MESH) for i in range(n - 1)]
    for c in out:
        c.start()
    buf[me] = x_ref[...]
    for i in range(n - 1):
        src = (me + n - 1 - i) % n
        pltpu.make_async_remote_copy(src_ref=x_ref, dst_ref=buf.at[src], send_sem=send.at[i], recv_sem=recv.at[i],
                                     device_id={'tp': peers[i]}, device_id_type=MESH).wait_recv()
    total = buf[0]
    for i in range(1, n):
        total = total + buf[i]
    out_ref[...] = total
    for c in out:
        c.wait_send()


def group_total(n, x):
    vmem = pl.BlockSpec(memory_space=pltpu.VMEM)
    return pl.pallas_call(
        functools.partial(total_kernel, n),
        in_specs=[vmem], out_specs=vmem, out_shape=jax.ShapeDtypeStruct(x.shape, x.dtype),
        scratch_shapes=[pltpu.VMEM((n,) + x.shape, x.dtype), pltpu.SemaphoreType.DMA((n - 1,)), pltpu.SemaphoreType.DMA((n - 1,))],
        compiler_params=comm_params(4), name="group_total",
    )(x)


def norm_kernel(post, u_ref, g_ref, x_ref, gain_ref, *outs):
    u = u_ref[...].astype(jnp.float32)
    cot = g_ref[...].astype(jnp.float32)
    gain = 1.0 + gain_ref[...]
    inv = lax.rsqrt(jnp.mean(u * u, axis=-1, keepdims=True) + NORM_EPS)
    xhat = u * inv
    if post:
        y_ref, d_ref, dg_ref = outs
        normed = (xhat * gain).astype(jnp.bfloat16).astype(jnp.float32)
        y_ref[...] = (x_ref[...].astype(jnp.float32) + normed).astype(jnp.bfloat16)
    else:
        d_ref, dg_ref = outs
    scaled = cot * gain
    d_u = (inv * (scaled - xhat * jnp.mean(scaled * xhat, axis=-1, keepdims=True))).astype(jnp.bfloat16)
    if post:
        d_ref[...] = d_u
    else:
        d_ref[...] = (x_ref[...].astype(jnp.float32) + d_u.astype(jnp.float32)).astype(jnp.bfloat16)

    @pl.when(pl.program_id(0) == 0)
    def _():
        dg_ref[...] = jnp.zeros_like(dg_ref)

    dg_ref[...] += jnp.sum(cot * xhat, axis=0, keepdims=True)


def norm_backward(post, u, cot, extra, gain):
    rows, d_model = u.shape
    tile = 64
    spec = pl.BlockSpec((tile, d_model), lambda i: (i, 0))
    one = pl.BlockSpec((1, d_model), lambda i: (0, 0))
    wide = jax.ShapeDtypeStruct(u.shape, jnp.bfloat16)
    return pl.pallas_call(
        functools.partial(norm_kernel, post),
        grid=(rows // tile,),
        in_specs=[spec] * 3 + [one],
        out_specs=[spec] * (2 if post else 1) + [one],
        out_shape=[wide] * (2 if post else 1) + [jax.ShapeDtypeStruct((1, d_model), jnp.float32)],
        compiler_params=params(),
        cost_estimate=pl.CostEstimate(flops=20 * u.size, transcendentals=0, bytes_accessed=10 * u.size),
        name="norm_backward",
    )(u, cot, extra, gain)


def solution(mesh):
    act_spec = P('dp', 'tp', None)
    head_spec = P(None, 'tp', None)
    grad_spec = P('dp', 'tp', None)
    in_specs = (act_spec, P('dp', 'tp'), act_spec, head_spec, head_spec, head_spec, P('tp', None, None), P(None), P(None))
    out_specs = (act_spec, act_spec, grad_spec, grad_spec, grad_spec, P(('dp', 'tp'), None, None), P('dp'), P('dp'))
    n_own = mesh.shape['tp']

    def local_step(x_in, positions, grad_out, w_query, w_key, w_value, w_out, gain_pre, gain_post):
        d_model, n_heads, hd = w_query.shape
        loc = x_in.shape[1]
        n_chunks = loc // ROWS
        scale = hd ** -0.5
        half = hd // 2
        qw = n_heads * hd
        w_cat = jnp.concatenate([w_query.reshape(d_model, qw), w_key.reshape(d_model, hd), w_value.reshape(d_model, hd)], axis=1)
        wo = w_out.reshape(qw, d_model)

        pos = lax.all_gather(positions, 'tp', axis=1, tiled=True).reshape(n_own, n_chunks, ROWS)
        inv_freq = ROPE_THETA ** (-2.0 * jnp.arange(half, dtype=jnp.float32) / hd)
        angles = pos.astype(jnp.float32)[..., None] * inv_freq
        cos_t, sin_t = jnp.cos(angles), jnp.sin(angles)
        pos_k = jnp.broadcast_to(pos.reshape(-1, ROWS, 1), (n_own * n_chunks, ROWS, ROWS))
        k_last = pos[:, :, -1].reshape(-1)
        lo = jnp.sum((pos[:, :, :1] - k_last >= WINDOW).astype(jnp.int32), axis=-1).reshape(-1)
        pos_q = pos[:, :, None]

        a_all, q_all, k_all, kt_all, v_all, vt_all = gather_qkv(n_own, n_heads, scale, x_in[0], gain_pre[None], w_cat, cos_t, sin_t)
        o, ot, qt, li = attn_fwd(n_heads, lo, q_all, k_all, vt_all, pos_q, pos_k)
        r, = matmul_scatter(n_own, 2, False, o.reshape(n_own, loc, qw), wo)
        y_out, d_proj, d_gain_post = norm_backward(True, r, grad_out[0], x_in[0], gain_post[None])
        do, grad_wo = gather_dproj(n_own, n_heads, d_proj, wo, ot)
        dcat = attn_bwd(n_heads, scale, lo, q_all, qt, ot, li, do, k_all, kt_all, v_all, pos_q, pos_k, cos_t, sin_t)
        da, grad_wq, grad_wk, grad_wv = matmul_scatter(n_own, 3, True, dcat.reshape(n_own, loc, qw + 2 * hd), w_cat,
                                                       a_all.reshape(n_own * loc, d_model), n_heads)
        grad_x, d_gain_pre = norm_backward(False, x_in[0], da, grad_out[0], gain_pre[None])
        gains = group_total(n_own, jnp.concatenate([d_gain_pre, d_gain_post], axis=0))
        return (y_out[None], grad_x[None], grad_wq, grad_wk, grad_wv, grad_wo.reshape(n_heads, hd, d_model), gains[0], gains[1])

    return jax.shard_map(local_step, mesh=mesh, in_specs=in_specs, out_specs=out_specs, check_vma=False)
```

```python
import functools

import jax
import jax.numpy as jnp
from jax import lax
from jax.experimental import pallas as pl
from jax.experimental.pallas import tpu as pltpu
from jax.sharding import PartitionSpec as P

WINDOW = 4096
SOFT_CAP = 50.0
NORM_EPS = 1e-6
ROPE_THETA = 10000.0
ROWS = 128
LOG2E = 1.4426950408889634
VMEM_LIMIT = 60 * 1024 * 1024
KEY_BLOCKS = 4


def rms_norm(hidden, scale_w):
    values = hidden.astype(jnp.float32)
    inv_rms = lax.rsqrt(jnp.mean(values * values, axis=-1, keepdims=True) + NORM_EPS)
    return (values * inv_rms * (1.0 + scale_w)).astype(jnp.bfloat16)


def as_row(ref):
    return jnp.concatenate([ref[i:i + 1] for i in range(ref.shape[0])], axis=1)


def params(n=1):
    return pltpu.CompilerParams(dimension_semantics=("arbitrary",) * n, vmem_limit_bytes=VMEM_LIMIT)


def key_mask(posq_ref, posk_ref, start, limit):
    keys = KEY_BLOCKS * ROWS
    gap = posq_ref[0, 0] - posk_ref[pl.ds(start, KEY_BLOCKS)].reshape(keys, ROWS)
    row = lax.broadcasted_iota(jnp.int32, (keys, ROWS), 0)
    return (gap >= 0) & (gap < WINDOW) & (row < limit)


def key_range(lo_ref, own, cur, n_chunks):
    end = own * n_chunks + cur + 1
    steps = (end - lo_ref[end - 1] + KEY_BLOCKS - 1) // KEY_BLOCKS

    def at(i):
        stop = end - KEY_BLOCKS * i
        start = jnp.maximum(stop - KEY_BLOCKS, 0)
        return start, (stop - start) * ROWS

    return steps, at


def side_by_side(ref, start):
    return jnp.concatenate([ref[start + c] for c in range(KEY_BLOCKS)], axis=1)


def masked_exp(t, mask, n_heads, shift=0.0):
    e = jnp.exp2(t * (SOFT_CAP * LOG2E) - shift)
    return jnp.concatenate([jnp.where(mask, e[:, h * ROWS:(h + 1) * ROWS], 0.0) for h in range(n_heads)], axis=1)


def fwd_kernel(n_heads, lo_ref, q_ref, k_ref, vt_ref, posq_ref, posk_ref, o_ref, ot_ref, qt_ref, li_ref, acc_ref):
    own, cur = pl.program_id(0), pl.program_id(1)
    n_chunks, hd = pl.num_programs(1), k_ref.shape[2]
    keys = KEY_BLOCKS * ROWS
    q = q_ref[0, 0]
    qt = jnp.concatenate([q[:, h * hd:(h + 1) * hd].T for h in range(n_heads)], axis=1)
    qt_ref[0, 0] = qt
    acc_ref[...] = jnp.zeros_like(acc_ref)

    steps, at = key_range(lo_ref, own, cur, n_chunks)

    def body(i, l_sum):
        start, limit = at(i)
        k_b = k_ref[pl.ds(start, KEY_BLOCKS)].reshape(keys, hd)
        s = jnp.dot(k_b, qt_ref[0, 0], preferred_element_type=jnp.float32)
        t = jnp.tanh(s * (1.0 / SOFT_CAP))
        e = masked_exp(t, key_mask(posq_ref, posk_ref, start, limit), n_heads)
        acc_ref[...] += jnp.dot(side_by_side(vt_ref, start), e.astype(jnp.bfloat16), preferred_element_type=jnp.float32)
        return l_sum + jnp.sum(e, axis=0, keepdims=True)

    l_sum = lax.fori_loop(0, steps, body, jnp.zeros((1, n_heads * ROWS), jnp.float32))
    inv = 1.0 / l_sum
    li_ref[0, 0] = jnp.log2(l_sum)
    ot = (acc_ref[...] * inv).astype(jnp.bfloat16)
    ot_ref[0, 0] = ot
    for h in range(n_heads):
        o_ref[0, 0, :, h * hd:(h + 1) * hd] = ot[:, h * ROWS:(h + 1) * ROWS].T


def attn_fwd(n_heads, lo, q, k, vt, posq, posk):
    n_own, n_chunks, rows = q.shape[:3]
    hd = k.shape[-1]
    lanes = n_heads * rows
    full = lambda x: pl.BlockSpec(x.shape, lambda i, c, lo: (0,) * x.ndim)
    per = lambda s: pl.BlockSpec((1, 1) + s, lambda i, c, lo: (i, c, 0, 0))
    out = lambda s, t: jax.ShapeDtypeStruct((n_own, n_chunks) + s, t)
    return pl.pallas_call(
        functools.partial(fwd_kernel, n_heads),
        grid_spec=pltpu.PrefetchScalarGridSpec(
            num_scalar_prefetch=1, grid=(n_own, n_chunks),
            in_specs=[per((rows, n_heads * hd)), full(k), full(vt), per((1, rows)), full(posk)],
            out_specs=[per((rows, n_heads * hd)), per((hd, lanes)), per((hd, lanes)), per((1, lanes))],
            scratch_shapes=[pltpu.VMEM((hd, lanes), jnp.float32)]),
        out_shape=[out((rows, n_heads * hd), jnp.bfloat16), out((hd, lanes), jnp.bfloat16),
                   out((hd, lanes), jnp.bfloat16), out((1, lanes), jnp.float32)],
        compiler_params=params(2),
        cost_estimate=pl.CostEstimate(flops=2 * q.size * n_own * n_chunks * rows, transcendentals=0, bytes_accessed=12 * k.size),
        name="attn_fwd",
    )(lo, q, k, vt, posq, posk)


def bwd_kernel(n_heads, scale, lo_ref, q_ref, qt_ref, ot_ref, li_ref, do_ref, k_ref, kt_ref, v_ref, posq_ref, posk_ref,
               cos_ref, sin_ref, out_ref, dk_ref, dv_ref, dqt_ref, dot_ref, dos_ref, qs_ref):
    own, cur = pl.program_id(0), pl.program_id(1)
    n_own, n_chunks, hd = pl.num_programs(0), pl.num_programs(1), k_ref.shape[2]
    keys = KEY_BLOCKS * ROWS
    half = hd // 2
    qw = n_heads * hd

    @pl.when((own == 0) & (cur == 0))
    def _():
        dk_ref[...] = jnp.zeros_like(dk_ref)
        dv_ref[...] = jnp.zeros_like(dv_ref)

    do = do_ref[0, 0]
    q = q_ref[0, 0]
    for h in range(n_heads):
        dos_ref[h * ROWS:(h + 1) * ROWS] = do[:, h * hd:(h + 1) * hd]
        qs_ref[h * ROWS:(h + 1) * ROWS] = q[:, h * hd:(h + 1) * hd]
        dot_ref[:, h * ROWS:(h + 1) * ROWS] = do[:, h * hd:(h + 1) * hd].T
    delta = jnp.sum(dot_ref[...].astype(jnp.float32) * ot_ref[0, 0].astype(jnp.float32), axis=0, keepdims=True)
    log_sum = li_ref[0, 0]
    dqt_ref[...] = jnp.zeros_like(dqt_ref)

    steps, at = key_range(lo_ref, own, cur, n_chunks)

    def body(i, carry):
        start, limit = at(i)
        here = pl.ds(start, KEY_BLOCKS)
        k_b = k_ref[here].reshape(keys, hd)
        v_b = v_ref[here].reshape(keys, hd)
        s = jnp.dot(k_b, qt_ref[0, 0], preferred_element_type=jnp.float32)
        dp = jnp.dot(v_b, dot_ref[...], preferred_element_type=jnp.float32)
        t = jnp.tanh(s * (1.0 / SOFT_CAP))
        p = masked_exp(t, key_mask(posq_ref, posk_ref, start, limit), n_heads, log_sum)
        ds = (p * (dp - delta) * (1.0 - t * t)).astype(jnp.bfloat16)
        dv_ref[here] += jnp.dot(p.astype(jnp.bfloat16), dos_ref[...], preferred_element_type=jnp.float32).reshape(KEY_BLOCKS, ROWS, hd)
        dk_ref[here] += jnp.dot(ds, qs_ref[...], preferred_element_type=jnp.float32).reshape(KEY_BLOCKS, ROWS, hd)
        dqt_ref[...] += jnp.dot(side_by_side(kt_ref, start), ds, preferred_element_type=jnp.float32)
        return carry

    lax.fori_loop(0, steps, body, 0)

    def unrope(grad, cos, sin):
        lo, hi = grad[:, :half], grad[:, half:]
        return lo * cos + hi * sin, hi * cos - lo * sin

    cos, sin = cos_ref[own, cur], sin_ref[own, cur]
    for h in range(n_heads):
        lo, hi = unrope(dqt_ref[:, h * ROWS:(h + 1) * ROWS].T, cos, sin)
        out_ref[own, cur, :, h * hd:h * hd + half] = (lo * scale).astype(jnp.bfloat16)
        out_ref[own, cur, :, h * hd + half:(h + 1) * hd] = (hi * scale).astype(jnp.bfloat16)

    @pl.when((own == n_own - 1) & (cur == n_chunks - 1))
    def _():
        def fin(i, carry):
            for c in range(out_ref.shape[1]):
                b = i * out_ref.shape[1] + c
                lo, hi = unrope(dk_ref[b], cos_ref[i, c], sin_ref[i, c])
                out_ref[i, c, :, qw:qw + half] = lo.astype(jnp.bfloat16)
                out_ref[i, c, :, qw + half:qw + hd] = hi.astype(jnp.bfloat16)
                out_ref[i, c, :, qw + hd:] = dv_ref[b].astype(jnp.bfloat16)
            return carry
        lax.fori_loop(0, n_own, fin, 0)


def attn_bwd(n_heads, scale, lo, q, qt, ot, li, do, k, kt, v, posq, posk, cos_t, sin_t):
    n_own, n_chunks, rows = q.shape[:3]
    hd = k.shape[-1]
    lanes = n_heads * rows
    once = dict(pipeline_mode=pl.Buffered(1))
    full = lambda x: pl.BlockSpec(x.shape, lambda i, c, lo: (0,) * x.ndim, **once)
    per = lambda s: pl.BlockSpec((1, 1) + s, lambda i, c, lo: (i, c, 0, 0))
    out = jax.ShapeDtypeStruct((n_own, n_chunks, rows, (n_heads + 2) * hd), jnp.bfloat16)
    acc = pltpu.VMEM(k.shape, jnp.float32)
    return pl.pallas_call(
        functools.partial(bwd_kernel, n_heads, scale),
        grid_spec=pltpu.PrefetchScalarGridSpec(
            num_scalar_prefetch=1, grid=(n_own, n_chunks),
            in_specs=[per((rows, n_heads * hd)), per((hd, lanes)), per((hd, lanes)), per((1, lanes)),
                      per((rows, n_heads * hd)), full(k), full(kt), full(v), per((1, rows)), full(posk),
                      full(cos_t), full(sin_t)],
            out_specs=pl.BlockSpec(out.shape, lambda i, c, lo: (0, 0, 0, 0)),
            scratch_shapes=[acc, acc, pltpu.VMEM((hd, lanes), jnp.float32), pltpu.VMEM((hd, lanes), jnp.bfloat16),
                            pltpu.VMEM((lanes, hd), jnp.bfloat16), pltpu.VMEM((lanes, hd), jnp.bfloat16)]),
        out_shape=out,
        compiler_params=params(2),
        cost_estimate=pl.CostEstimate(flops=5 * q.size * n_own * n_chunks * rows, transcendentals=0, bytes_accessed=24 * k.size),
        name="attn_bwd",
    )(lo, q, qt, ot, li, do, k, kt, v, posq, posk, cos_t, sin_t)


MESH = pl.DeviceIdType.MESH


def ring_ids(n):
    me = lax.axis_index('tp')
    return me, me + 1 - 2 * (me % 2), (me + 2) % n, (me + n - 2) % n


def greet(peers):
    barrier = pltpu.get_barrier_semaphore()
    for peer in peers:
        pl.semaphore_signal(barrier, inc=1, device_id={'tp': peer}, device_id_type=MESH)
    pl.semaphore_wait(barrier, len(peers))


def comm_params(cid):
    return pltpu.CompilerParams(collective_id=cid, has_side_effects=True, vmem_limit_bytes=63 * 1024 * 1024)


def gather_ring(n, src_ref, all_ref, send, recv, compute):
    me, partner, right, left = ring_ids(n)
    opp = (me + n // 2) % n
    half = src_ref.shape[0] // 2

    def part(owner, h):
        return all_ref.at[owner, pl.ds(h * half, half)]

    def copy(idx, src, owner, h, target):
        return pltpu.make_async_remote_copy(src_ref=src, dst_ref=part(owner, h), send_sem=send.at[idx], recv_sem=recv.at[idx],
                                            device_id={'tp': target}, device_id_type=MESH)

    def own(idx, h, target):
        return copy(idx, src_ref.at[pl.ds(h * half, half)], me, h, target)

    def fwd(idx, owner, h, target):
        return copy(idx, part(owner, h), owner, h, target)

    def arrived(idx, owner, h):
        fwd(idx, owner, h, partner).wait_recv()

    firsts = [own(0, 0, right), own(2, 1, left), own(1, 1, right), own(3, 0, left), own(4, 0, partner), own(5, 1, partner)]
    for c in firsts:
        c.start()
    all_ref[me] = src_ref[...]
    relays = [fwd(6, left, 0, right), fwd(7, right, 1, left), fwd(8, left, 0, partner), fwd(9, left, 1, partner),
              fwd(10, right, 1, partner), fwd(11, right, 0, partner), fwd(12, opp, 0, partner), fwd(13, opp, 1, partner)]
    l_par, r_par, o_par = (partner + n - 2) % n, (partner + 2) % n, (partner + n // 2) % n
    order = (me, partner, left, right, l_par, r_par, opp, o_par)

    def step(i, carry):
        @pl.when(i == 1)
        def _():
            arrived(4, partner, 0)
            arrived(5, partner, 1)

        @pl.when(i == 2)
        def _():
            arrived(0, left, 0)
            relays[0].start()
            relays[2].start()
            arrived(2, right, 1)
            relays[1].start()
            relays[4].start()
            arrived(1, left, 1)
            relays[3].start()

        @pl.when(i == 3)
        def _():
            arrived(3, right, 0)
            relays[5].start()

        @pl.when(i == 4)
        def _():
            arrived(8, l_par, 0)
            arrived(9, l_par, 1)

        @pl.when(i == 5)
        def _():
            arrived(10, r_par, 1)
            arrived(11, r_par, 0)

        @pl.when(i == 6)
        def _():
            arrived(6, opp, 0)
            relays[6].start()
            arrived(7, opp, 1)
            relays[7].start()

        @pl.when(i == 7)
        def _():
            arrived(12, o_par, 0)
            arrived(13, o_par, 1)

        owner = order[0]
        for j in range(1, len(order)):
            owner = jnp.where(i == j, order[j], owner)
        compute(owner)
        return carry

    lax.fori_loop(0, n, step, 0)
    for c in firsts + relays:
        c.wait_send()


def gather_scratch(n, rows, d_model):
    return [pltpu.VMEM((n, rows, d_model), jnp.bfloat16), pltpu.SemaphoreType.DMA((14,)), pltpu.SemaphoreType.DMA((14,))]


def qkv_kernel(n, n_heads, scale, x_ref, gain_ref, wq_ref, wk_ref, wv_ref, cos_ref, sin_ref, a_ref, q_ref, k_ref, kt_ref, v_ref, vt_ref,
               own_ref, all_ref, send, recv, out_sem):
    rows = x_ref.shape[0]
    n_chunks, half = cos_ref.shape[1], cos_ref.shape[3]
    hd = 2 * half
    own_ref[...] = rms_norm(x_ref[...], as_row(gain_ref))
    _, partner, right, left = ring_ids(n)
    greet((partner, right, left))

    def to_hbm(owner):
        return pltpu.make_async_copy(all_ref.at[owner], a_ref.at[owner], out_sem.at[owner])

    def compute(owner):
        to_hbm(owner).start()
        a = all_ref[owner]
        q_lin = jnp.dot(a, wq_ref[...], preferred_element_type=jnp.float32)
        k_lin = jnp.dot(a, wk_ref[...], preferred_element_type=jnp.float32)
        v = jnp.dot(a, wv_ref[...], preferred_element_type=jnp.float32).astype(jnp.bfloat16)
        cos = cos_ref[owner].reshape(rows, half)
        sin = sin_ref[owner].reshape(rows, half)

        def rope(lin, col):
            lo = lin[:, col:col + half]
            hi = lin[:, col + half:col + hd]
            return lo * cos - hi * sin, hi * cos + lo * sin

        for h in range(n_heads):
            lo, hi = rope(q_lin, h * hd)
            q_ref[owner, :, :, h * hd:h * hd + half] = (lo * scale).astype(jnp.bfloat16).reshape(n_chunks, ROWS, half)
            q_ref[owner, :, :, h * hd + half:(h + 1) * hd] = (hi * scale).astype(jnp.bfloat16).reshape(n_chunks, ROWS, half)
        lo, hi = rope(k_lin, 0)
        k = jnp.concatenate([lo.astype(jnp.bfloat16), hi.astype(jnp.bfloat16)], axis=1)
        for c in range(n_chunks):
            b = owner * n_chunks + c
            k_c = k[c * ROWS:(c + 1) * ROWS]
            v_c = v[c * ROWS:(c + 1) * ROWS]
            k_ref[b] = k_c
            kt_ref[b] = k_c.T
            v_ref[b] = v_c
            vt_ref[b] = v_c.T

    gather_ring(n, own_ref, all_ref, send, recv, compute)

    def drain(i, carry):
        to_hbm(i).wait()
        return carry

    lax.fori_loop(0, n, drain, 0)


def gather_qkv(n, n_heads, scale, x, gain, ws, cos_t, sin_t):
    rows, d_model = x.shape
    n_chunks, hd = cos_t.shape[1], 2 * cos_t.shape[3]
    blocks = n * n_chunks
    bf = lambda s: jax.ShapeDtypeStruct(s, jnp.bfloat16)
    vmem = pl.BlockSpec(memory_space=pltpu.VMEM)
    return pl.pallas_call(
        functools.partial(qkv_kernel, n, n_heads, scale),
        in_specs=[vmem] * 7, out_specs=[pl.BlockSpec(memory_space=pl.ANY)] + [vmem] * 5,
        out_shape=[bf((n, rows, d_model)), bf((n, n_chunks, ROWS, n_heads * hd)),
                   bf((blocks, ROWS, hd)), bf((blocks, hd, ROWS)), bf((blocks, ROWS, hd)), bf((blocks, hd, ROWS))],
        scratch_shapes=[pltpu.VMEM((rows, d_model), jnp.bfloat16)] + gather_scratch(n, rows, d_model) + [pltpu.SemaphoreType.DMA((n,))],
        compiler_params=comm_params(0),
        cost_estimate=pl.CostEstimate(flops=2 * n * x.size * (n_heads + 2) * hd, transcendentals=0, bytes_accessed=4 * n * x.size),
        name="gather_qkv",
    )(x, gain, *ws, cos_t, sin_t)


def dproj_kernel(n, n_heads, x_ref, wo_ref, ot_ref, do_ref, gwo_ref, all_ref, send, recv):
    n_chunks, hd = ot_ref.shape[1], ot_ref.shape[2]
    _, partner, right, left = ring_ids(n)
    greet((partner, right, left))
    gwo_ref[...] = jnp.zeros_like(gwo_ref)

    def compute(owner):
        dp = all_ref[owner]
        do = lax.dot_general(dp, wo_ref[...], (((1,), (1,)), ((), ())), preferred_element_type=jnp.float32)
        do_ref[owner] = do.astype(jnp.bfloat16).reshape(n_chunks, ROWS, n_heads * hd)
        for h in range(n_heads):
            ot = jnp.concatenate([ot_ref[owner, c, :, h * ROWS:(h + 1) * ROWS] for c in range(n_chunks)], axis=1)
            gwo_ref[h * hd:(h + 1) * hd] += jnp.dot(ot, dp, preferred_element_type=jnp.float32)

    gather_ring(n, x_ref, all_ref, send, recv, compute)


def gather_dproj(n, n_heads, d_proj, wo, ot):
    rows, d_model = d_proj.shape
    n_chunks, hd = ot.shape[1], ot.shape[2]
    vmem = pl.BlockSpec(memory_space=pltpu.VMEM)
    return pl.pallas_call(
        functools.partial(dproj_kernel, n, n_heads),
        in_specs=[vmem] * 3, out_specs=[vmem] * 2,
        out_shape=[jax.ShapeDtypeStruct((n, n_chunks, ROWS, n_heads * hd), jnp.bfloat16),
                   jax.ShapeDtypeStruct((n_heads * hd, d_model), jnp.float32)],
        scratch_shapes=gather_scratch(n, rows, d_model),
        compiler_params=comm_params(1),
        cost_estimate=pl.CostEstimate(flops=4 * n * rows * d_model * n_heads * hd, transcendentals=0, bytes_accessed=2 * n * d_proj.size),
        name="gather_dproj",
    )(d_proj, wo, ot)


def scatter_kernel(n, pieces, n_heads, *refs):
    if n_heads:
        lhs_ref, wq_ref, wk_ref, wv_ref, a_ref, out_ref, gq_ref, gk_ref, gv_ref = refs[:9]
        a_buf, g_bufs, a_sem, g_sem = refs[-6], refs[-5:-2], refs[-2], refs[-1]
        acc, pst, pin, rcv, p_send, p_recv, r_send, r_recv = refs[9:-6]
    else:
        lhs_ref, rhs_ref, out_ref, acc, pst, pin, rcv, p_send, p_recv, r_send, r_recv = refs
    me, partner, right, left = ring_ids(n)
    core = me % 2
    chips = n // 2
    chip = me // 2
    width = acc.shape[2]
    rows = acc.shape[1]
    prow = rows // pieces
    hop = (right, left)
    greet((partner, right, left))

    if n_heads:
        tile = a_buf.shape[2]
        hd = gk_ref.shape[2]
        tiles = a_ref.shape[1] // tile
        per_stage = tiles // (chips - 1)
        depth = lhs_ref.shape[2]

        def a_in(t):
            return pltpu.make_async_copy(a_ref.at[:, pl.ds(pl.multiple_of(t * tile, tile), tile)], a_buf.at[t % 2], a_sem.at[t % 2])

        def g_out(t):
            at = pl.ds(pl.multiple_of(t * tile, tile), tile)
            return [pltpu.make_async_copy(b.at[t % 2], g.at[at], g_sem.at[t % 2, i])
                    for i, (b, g) in enumerate(zip(g_bufs, (gq_ref, gk_ref, gv_ref)))]

        def wgrad(t, carry):
            a_in(t).wait()

            @pl.when(t + 1 < tiles)
            def _():
                a_in(t + 1).start()

            @pl.when(t >= 2)
            def _():
                for c in g_out(t - 2):
                    c.wait()

            g = lax.dot_general(a_buf[t % 2], lhs_ref[...].reshape(n * rows, depth), (((0,), (0,)), ((), ())),
                                preferred_element_type=jnp.float32)
            for h in range(n_heads):
                g_bufs[0][t % 2, :, h, :] = g[:, h * hd:(h + 1) * hd]
            g_bufs[1][t % 2, :, 0, :] = g[:, n_heads * hd:(n_heads + 1) * hd]
            g_bufs[2][t % 2, :, 0, :] = g[:, (n_heads + 1) * hd:]
            for c in g_out(t):
                c.start()
            return carry

        a_in(0).start()

    def partial_sum(owner, d):
        if n_heads:
            total, col = None, 0
            for w_ref in (wq_ref, wk_ref, wv_ref):
                part = lax.dot_general(lhs_ref[owner, :, col:col + w_ref.shape[1]], w_ref[d * width:(d + 1) * width],
                                       (((1,), (1,)), ((), ())), preferred_element_type=jnp.float32)
                total = part if total is None else total + part
                col += w_ref.shape[1]
            return total
        return jnp.dot(lhs_ref[owner], rhs_ref[:, d * width:(d + 1) * width], preferred_element_type=jnp.float32)

    def to_partner(j, d):
        return pltpu.make_async_remote_copy(src_ref=pst.at[j % 2, d], dst_ref=pin.at[j, d], send_sem=p_send.at[j, d],
                                            recv_sem=p_recv.at[j, d], device_id={'tp': partner}, device_id_type=MESH)

    def to_next(j, d, p):
        at = pl.ds(p * prow, prow)
        return pltpu.make_async_remote_copy(src_ref=pin.at[j, d, at], dst_ref=rcv.at[j, d, at], send_sem=r_send.at[j, d, p],
                                            recv_sem=r_recv.at[j, d, p], device_id={'tp': hop[d]}, device_id_type=MESH)

    def stage(j, carry):
        dest = ((chip + 2 * chips - 1 - j) % chips, (chip + 1 + j) % chips)

        @pl.when(j >= 2)
        def _():
            for d in range(2):
                to_partner(j - 2, d).wait_send()

        for d in range(2):
            pst[j % 2, d] = partial_sum(dest[d] * 2 + 1 - core, d).astype(jnp.bfloat16)
            to_partner(j, d).start()
        for d in range(2):
            acc[d] = partial_sum(dest[d] * 2 + core, d)
        for d in range(2):
            to_partner(j, d).wait_recv()
        for p in range(pieces):
            at = slice(p * prow, (p + 1) * prow)
            for d in range(2):
                @pl.when(j == 0)
                def _():
                    pin[0, d, at] = (acc[d, at] + pin[0, d, at].astype(jnp.float32)).astype(jnp.bfloat16)
                    to_next(0, d, p).start()

                @pl.when((j > 0) & (j < chips - 1))
                def _():
                    to_next(j - 1, d, p).wait_recv()
                    pin[j, d, at] = (acc[d, at] + pin[j, d, at].astype(jnp.float32)
                                     + rcv[j - 1, d, at].astype(jnp.float32)).astype(jnp.bfloat16)
                    to_next(j, d, p).start()

                @pl.when(j == chips - 1)
                def _():
                    to_next(chips - 2, d, p).wait_recv()
                    out_ref[at, d * width:(d + 1) * width] = (
                        acc[d, at] + pin[chips - 1, d, at].astype(jnp.float32)
                        + rcv[chips - 2, d, at].astype(jnp.float32)).astype(jnp.bfloat16)
        if n_heads:
            first = jnp.minimum(j * per_stage, tiles)
            lax.fori_loop(first, jnp.minimum(first + per_stage, tiles), wgrad, 0)
        return carry

    lax.fori_loop(0, chips, stage, 0)
    if n_heads:
        for t in (tiles - 2, tiles - 1):
            for c in g_out(t):
                c.wait()
    for d in range(2):
        for j in (chips - 2, chips - 1):
            to_partner(j, d).wait_send()
        for j in range(chips - 1):
            for p in range(pieces):
                to_next(j, d, p).wait_send()


def matmul_scatter(n, cid, lhs, weights, d_model, a=None, n_heads=0):
    rows, depth = lhs.shape[1:]
    chips, width, pieces = n // 2, d_model // 2, 3
    vmem = pl.BlockSpec(memory_space=pltpu.VMEM)
    hbm = pl.BlockSpec(memory_space=pl.ANY)
    bf = lambda k: pltpu.VMEM((k, 2, rows, width), jnp.bfloat16)
    dma = pltpu.SemaphoreType.DMA
    out_shape = [jax.ShapeDtypeStruct((rows, d_model), jnp.bfloat16)]
    scratch = [pltpu.VMEM((2, rows, width), jnp.float32), bf(2), bf(chips), bf(chips - 1),
               dma((chips, 2)), dma((chips, 2)), dma((chips - 1, 2, pieces)), dma((chips - 1, 2, pieces))]
    args = [lhs, *weights]
    flops = 2 * n * rows * depth * d_model
    if n_heads:
        hd, tile = depth // (n_heads + 2), 256
        args.append(a)
        out_shape += [jax.ShapeDtypeStruct((d_model, k, hd), jnp.float32) for k in (n_heads, 1, 1)]
        scratch += [pltpu.VMEM((2, n * rows, tile), jnp.bfloat16)]
        scratch += [pltpu.VMEM((2, tile, k, hd), jnp.float32) for k in (n_heads, 1, 1)] + [dma((2,)), dma((2, 3))]
        flops *= 2
    return pl.pallas_call(
        functools.partial(scatter_kernel, n, pieces, n_heads),
        in_specs=[vmem] * (1 + len(weights)) + [hbm] * (len(args) - 1 - len(weights)), out_specs=[vmem] + [hbm] * (len(out_shape) - 1),
        out_shape=out_shape,
        scratch_shapes=scratch,
        compiler_params=comm_params(cid),
        cost_estimate=pl.CostEstimate(flops=flops, transcendentals=0, bytes_accessed=2 * n * rows * d_model),
        name="matmul_scatter",
    )(*args)


def exchange(n, src_ref, buf, send, recv):
    me = lax.axis_index('tp')
    peers = [(me + i) % n for i in range(1, n)]
    greet(peers)

    def copy(i, slot):
        return pltpu.make_async_remote_copy(src_ref=src_ref, dst_ref=buf.at[slot], send_sem=send.at[i], recv_sem=recv.at[i],
                                            device_id={'tp': peers[i]}, device_id_type=MESH)

    out = [copy(i, me) for i in range(n - 1)]
    for c in out:
        c.start()
    buf[me] = src_ref[...]
    for i in range(n - 1):
        copy(i, (me + n - 1 - i) % n).wait_recv()
    for c in out:
        c.wait_send()


def total_kernel(n, a_ref, b_ref, a_out, b_out, src, buf, send, recv):
    src[0:1] = a_ref[...]
    src[1:2] = b_ref[...]
    exchange(n, src, buf, send, recv)
    total = buf[0]
    for i in range(1, n):
        total = total + buf[i]
    for i in range(a_out.shape[0]):
        a_out[i:i + 1] = total[0:1, i * 128:(i + 1) * 128]
        b_out[i:i + 1] = total[1:2, i * 128:(i + 1) * 128]


def positions_kernel(n, x_ref, out_ref, buf, send, recv):
    exchange(n, x_ref, buf, send, recv)
    out_ref[...] = buf[...]


def exchange_call(n, cid, kernel, args, outs, shape, dtype, extra, name):
    vmem = pl.BlockSpec(memory_space=pltpu.VMEM)
    dma = pltpu.SemaphoreType.DMA((n - 1,))
    return pl.pallas_call(
        functools.partial(kernel, n), in_specs=[vmem] * len(args), out_specs=[vmem] * len(outs), out_shape=outs,
        scratch_shapes=extra + [pltpu.VMEM((n,) + shape, dtype), dma, dma],
        compiler_params=comm_params(cid), name=name,
    )(*args)


def group_total(n, a, b):
    shape = (2, a.shape[1])
    out = jax.ShapeDtypeStruct((a.shape[1] // 128, 128), a.dtype)
    return exchange_call(n, 4, total_kernel, [a, b], [out] * 2, shape, a.dtype, [pltpu.VMEM(shape, a.dtype)], "group_total")


def gather_positions(n, pos):
    out = jax.ShapeDtypeStruct((n,) + pos.shape, pos.dtype)
    return exchange_call(n, 5, positions_kernel, [pos], [out], pos.shape, pos.dtype, [], "gather_positions")[0]


def norm_kernel(post, u_ref, g_ref, x_ref, gain_ref, *outs):
    u = u_ref[...].astype(jnp.float32)
    cot = g_ref[...].astype(jnp.float32)
    gain = 1.0 + as_row(gain_ref)
    inv = lax.rsqrt(jnp.mean(u * u, axis=-1, keepdims=True) + NORM_EPS)
    xhat = u * inv
    if post:
        y_ref, d_ref, dg_ref = outs
        normed = (xhat * gain).astype(jnp.bfloat16).astype(jnp.float32)
        y_ref[...] = (x_ref[...].astype(jnp.float32) + normed).astype(jnp.bfloat16)
    else:
        d_ref, dg_ref = outs
    scaled = cot * gain
    d_u = (inv * (scaled - xhat * jnp.mean(scaled * xhat, axis=-1, keepdims=True))).astype(jnp.bfloat16)
    if post:
        d_ref[...] = d_u
    else:
        d_ref[...] = (x_ref[...].astype(jnp.float32) + d_u.astype(jnp.float32)).astype(jnp.bfloat16)

    @pl.when(pl.program_id(0) == 0)
    def _():
        dg_ref[...] = jnp.zeros_like(dg_ref)

    dg_ref[...] += jnp.sum(cot * xhat, axis=0, keepdims=True)


def norm_backward(post, u, cot, extra, gain):
    rows, d_model = u.shape
    tile = 64
    spec = pl.BlockSpec((tile, d_model), lambda i: (i, 0))
    one = pl.BlockSpec((1, d_model), lambda i: (0, 0))
    wide = jax.ShapeDtypeStruct(u.shape, jnp.bfloat16)
    return pl.pallas_call(
        functools.partial(norm_kernel, post),
        grid=(rows // tile,),
        in_specs=[spec] * 3 + [pl.BlockSpec(gain.shape, lambda i: (0, 0))],
        out_specs=[spec] * (2 if post else 1) + [one],
        out_shape=[wide] * (2 if post else 1) + [jax.ShapeDtypeStruct((1, d_model), jnp.float32)],
        compiler_params=params(),
        cost_estimate=pl.CostEstimate(flops=20 * u.size, transcendentals=0, bytes_accessed=10 * u.size),
        name="norm_backward",
    )(u, cot, extra, gain)


def solution(mesh):
    act_spec = P('dp', 'tp', None)
    head_spec = P(None, 'tp', None)
    grad_spec = P('dp', 'tp', None)
    in_specs = (act_spec, P('dp', 'tp'), act_spec, head_spec, head_spec, head_spec, P('tp', None, None), P(None), P(None))
    out_specs = (act_spec, act_spec, grad_spec, grad_spec, grad_spec, P(('dp', 'tp'), None, None), P('dp'), P('dp'))
    n_own = mesh.shape['tp']

    def local_step(x_in, positions, grad_out, w_query, w_key, w_value, w_out, gain_pre, gain_post):
        d_model, n_heads, hd = w_query.shape
        loc = x_in.shape[1]
        n_chunks = loc // ROWS
        scale = hd ** -0.5
        half = hd // 2
        qw = n_heads * hd
        ws = [w_query.reshape(d_model, qw), w_key.reshape(d_model, hd), w_value.reshape(d_model, hd)]
        wo = w_out.reshape(qw, d_model)

        pos = gather_positions(n_own, positions).reshape(n_own, n_chunks, ROWS)
        inv_freq = ROPE_THETA ** (-2.0 * jnp.arange(half, dtype=jnp.float32) / hd)
        angles = pos.astype(jnp.float32)[..., None] * inv_freq
        cos_t, sin_t = jnp.cos(angles), jnp.sin(angles)
        pos_k = jnp.broadcast_to(pos.reshape(-1, ROWS, 1), (n_own * n_chunks, ROWS, ROWS))
        k_last = pos[:, :, -1].reshape(-1)
        lo = jnp.sum((pos[:, :, :1] - k_last >= WINDOW).astype(jnp.int32), axis=-1).reshape(-1)
        pos_q = pos[:, :, None]

        a_all, q_all, k_all, kt_all, v_all, vt_all = gather_qkv(n_own, n_heads, scale, x_in[0], gain_pre.reshape(-1, 128), ws, cos_t, sin_t)
        o, ot, qt, li = attn_fwd(n_heads, lo, q_all, k_all, vt_all, pos_q, pos_k)
        r, = matmul_scatter(n_own, 2, o.reshape(n_own, loc, qw), [wo], d_model)
        y_out, d_proj, d_gain_post = norm_backward(True, r, grad_out[0], x_in[0], gain_post.reshape(-1, 128))
        do, grad_wo = gather_dproj(n_own, n_heads, d_proj, wo, ot)
        dcat = attn_bwd(n_heads, scale, lo, q_all, qt, ot, li, do, k_all, kt_all, v_all, pos_q, pos_k, cos_t, sin_t)
        da, grad_wq, grad_wk, grad_wv = matmul_scatter(n_own, 3, dcat.reshape(n_own, loc, qw + 2 * hd), ws, d_model,
                                                       a_all.reshape(n_own * loc, d_model), n_heads)
        grad_x, d_gain_pre = norm_backward(False, x_in[0], da, grad_out[0], gain_pre.reshape(-1, 128))
        sum_pre, sum_post = group_total(n_own, d_gain_pre, d_gain_post)
        return (y_out[None], grad_x[None], grad_wq, grad_wk, grad_wv, grad_wo.reshape(n_heads, hd, d_model), sum_pre.reshape(-1), sum_post.reshape(-1))

    return jax.shard_map(local_step, mesh=mesh, in_specs=in_specs, out_specs=out_specs, check_vma=False)
```
